32 devices in a mesh: fluid: 8 (over y, x, core), solid: 4 (over z).
Axes of the slice: x: 2, y: 2, z: 4, core: 2. Of those that a mesh axis runs over, the one named last changes fastest.
Arguments:
- rbf_blocks: bfloat16 [3328, 256, 256], P(('fluid', 'solid')), may hold values from -0.375 to 0.375
- fluid_traction: bfloat16 [3328, 768], P(('fluid', 'solid')), may hold values from -24 to 24
- fluid_mass: bfloat16 [3328, 768], P(('fluid', 'solid')), may hold values from 0.19921875 to 2
- route: int32 [3328, 1], P(('fluid', 'solid')), may hold values from 0 to 31; in each aligned block of 104 rows (0 to 103, 104 to 207, ...) at most 6 rows name the same one
- slot: int32 [3328], P(('fluid', 'solid')), may hold values from 0 to 7
- shell_inverse: bfloat16 [256, 768, 768], P(('fluid', 'solid')), may hold values from -0.0078125 to 0.0078125
- robin_coef: float32 [256, 768], P(('fluid', 'solid')), may hold values from 1 to 27
- shell_start: float32 [256, 768], P(('fluid', 'solid')), may hold values from -3 to 3
Outputs:
- shell_displacement: float32 [256, 768], P(('fluid', 'solid'))
- fluid_load: bfloat16 [3328, 768], P(('fluid', 'solid'))
- residual_norms: float32 [6], replicated
The draws below stay inside these ranges and needn't reach their ends.
Inputs may be any that keep to these rules, and one draw needn't show every extreme that they name: `route`: among the 104 blocks of one device at most 6 name the same owner device.
All inputs are finite; a program needn't handle non-finite values.
Results may differ from the reference program's by a relative error of at most 0.009.
Values may be sent and summed in bfloat16 or wider, within the bound.
A program may use at most 128 MiB of HBM per device.

```python
import math
import jax
import jax.numpy as jnp
import numpy as np
from jax import lax

NODES = 256
FB_DEV = 104
SB_DEV = 8
ITERS = 6
CAP = 6
NFB = 3328
NSB = 256
N_FLUID = 8
N_SOLID = 4
DEVICES = 32


def place_ends(drawn, key, least, top_value):
    spot = [jax.random.randint(jax.random.fold_in(key, axis), (), 0, length) for axis, length in enumerate(drawn.shape)]
    widest = drawn.shape.index(max(drawn.shape))
    beside = spot[:widest] + [(spot[widest] + 1) % drawn.shape[widest]] + spot[widest + 1:]
    return drawn.at[tuple(spot)].set(least).at[tuple(beside)].set(top_value)


def level_of(key, extent, cuts, least, largest):
    loudness, own = 1.0, jax.random.fold_in(key, 6)
    for position, shards_of in cuts:
        draws = jnp.exp(jax.random.uniform(jax.random.fold_in(own, position), (shards_of,), jnp.float32, least / len(cuts), largest / len(cuts)))
        loudness = loudness * jnp.repeat(draws, extent[position] // shards_of).reshape([-1 if axis == position else 1 for axis in range(len(extent))])
    return loudness


def routed_block(rng, own, number, rows, amount, top, limit, slope):
    order = jax.random.permutation(rng, amount)
    crowded, ordinary = load_shares(amount, rows * top, limit, slope, True), load_shares(amount, rows * top, limit, slope, False)
    places = jnp.arange(amount)

    def named(tallies, offset_by):
        used = int((tallies > 0).sum())
        fixed = max(1, used // 4)
        moved = fixed + (places - fixed + offset_by * (used - fixed)) % max(1, amount - fixed)
        return jnp.zeros((amount,), jnp.int32).at[order[jnp.where(places < fixed, places, moved)]].set(jnp.asarray(tallies, jnp.int32))

    tallies = jnp.where(number % 4 == 0, named(crowded, number // 4), named(ordinary, number - number // 4 - 1))
    mixed = jax.random.permutation(jax.random.fold_in(own, 3), amount)
    giver, taker = mixed[0:amount // 2 * 2:2], mixed[1:amount // 2 * 2:2]
    slack = jnp.minimum(tallies[giver] - 1, limit - tallies[taker]) // 2
    slack = jnp.where((giver == order[0]) | (taker == order[0]) | (tallies[taker] == 0), 0, jnp.maximum(slack, 0))
    moved = jax.random.randint(jax.random.fold_in(own, 4), (amount // 2,), 0, 1 << 20) % (slack + 1)
    tallies = tallies.at[giver].add(-moved).at[taker].add(moved)
    members = jnp.searchsorted(jnp.cumsum(tallies), jnp.arange(rows * top), side="right").astype(jnp.int32)
    listing = members.reshape(top, rows).T
    listing = listing[jax.random.permutation(jax.random.fold_in(own, 1), rows)]
    offset_by = jax.random.randint(jax.random.fold_in(own, 2), (rows, 1), 0, top)
    return jnp.take_along_axis(listing, (jnp.arange(top)[None, :] + offset_by) % top, axis=1)


def load_shares(amount, total, reach, lean, full):
    portions = [(1 << 20) // math.isqrt(standing ** lean) + 1 for standing in range(1, amount + 1)]
    largest = reach if full else min(reach, max(-(-total // amount), total * portions[0] // sum(portions)))
    least = 1 if total - largest >= amount - 1 else 0
    counts, rest = [largest] + [least] * (amount - 1), total - largest - least * (amount - 1)
    while rest > 0:
        free = [i for i in range(1, amount) if counts[i] < largest] or [i for i in range(1, amount) if counts[i] < reach]
        mass, left = sum([portions[i] for i in free]), rest
        for i in free:
            extra = min(reach - counts[i], max(1, left * portions[i] // mass), rest)
            counts[i] = counts[i] + extra
            rest = rest - extra
    return np.array(counts)


def noise(own_key, dims, scale, bound, split=(), kind=jnp.bfloat16):
    drawn = scale * jax.random.normal(own_key, dims, jnp.float32)
    if split:
        drawn = drawn * level_of(own_key, dims, split, -0.22, 0.18)
    return jnp.clip(drawn, -bound, bound).astype(kind)


def setup_inputs(seed: int = 0) -> dict:
    splits = jax.random.split(jax.random.key(seed), 9)
    rbf_blocks = noise(splits[0], (NFB, NODES, NODES), NODES ** -0.5, 0.375, ((0, 32),))
    fluid_traction = noise(splits[1], (NFB, 3 * NODES), 4.0, 24.0, ((0, 32),))
    fluid_mass = jnp.clip(jnp.exp(math.log(2.0) - 2.306499 * jax.random.uniform(splits[2], (NFB, 3 * NODES), jnp.float32) ** level_of(splits[2], (NFB, 3 * NODES), ((0, 32),), -0.2, 0.2)), 0.19921875, 2.0).astype(jnp.bfloat16)
    route_keys = jax.random.split(jax.random.fold_in(splits[3], 1), NFB // FB_DEV)
    route_turns = jax.random.permutation(jax.random.fold_in(splits[3], 3), NFB // FB_DEV)
    route = jax.vmap(lambda own, number: routed_block(jax.random.fold_in(splits[3], 2), own, number, FB_DEV, DEVICES, 1, CAP, 0))(route_keys, route_turns).reshape((NFB, 1))
    slot = place_ends(jax.random.randint(splits[4], (NFB,), 0, SB_DEV), jax.random.fold_in(splits[4], 1), 0, SB_DEV - 1).astype(jnp.int32)
    shell_inverse = noise(splits[5], (NSB, 3 * NODES, 3 * NODES), (3 * NODES * 64 * FB_DEV // SB_DEV) ** -0.5, 0.0078125, ((0, 32),))
    robin_coef = jnp.clip(jnp.exp(math.log(27.0) - 3.295837 * jax.random.uniform(splits[6], (NSB, 3 * NODES), jnp.float32) ** level_of(splits[6], (NSB, 3 * NODES), ((0, 32),), -0.2, 0.2)), 1.0, 27.0)
    shell_start = noise(splits[7], (NSB, 3 * NODES), 0.5, 3.0, ((0, 32),), jnp.float32)
    return {"rbf_blocks": rbf_blocks, "fluid_traction": fluid_traction, "fluid_mass": fluid_mass, "route": route, "slot": slot, "shell_inverse": shell_inverse, "robin_coef": robin_coef, "shell_start": shell_start}


RELAX = 0.3
EPSILON = 1e-06

def fluid_side(pieces):
    hblock, displaced, traction, massive = pieces
    hfloat = hblock.astype(jnp.float32)
    moved = jnp.einsum('bcj,bij->bci', displaced.reshape(-1, 3, NODES).astype(jnp.float32), hfloat).reshape(-1, 3 * NODES)
    load = (traction.astype(jnp.float32) - massive.astype(jnp.float32) * moved).astype(jnp.bfloat16)
    mapped = jnp.einsum('bci,bij->bcj', load.reshape(-1, 3, NODES).astype(jnp.float32), hfloat).reshape(-1, 3 * NODES)
    return (load, mapped.astype(jnp.bfloat16))

def shell_side(pieces):
    inverse, forcing = pieces
    return jnp.einsum('bi,bij->bj', forcing.astype(jnp.float32), inverse.astype(jnp.float32))

def least_squares(gram, target_side):
    order = gram.shape[0]
    lower = [[None] * order for _ in range(order)]
    for row in range(order):
        for column in range(row + 1):
            total = gram[row, column]
            for inner in range(column):
                total = total - lower[row][inner] * lower[column][inner]
            if row == column:
                lower[row][row] = jnp.sqrt(total)
            else:
                lower[row][column] = total / lower[column][column]
    middle = []
    for row in range(order):
        total = target_side[row]
        for inner in range(row):
            total = total - lower[row][inner] * middle[inner]
        middle.append(total / lower[row][row])
    result = [None] * order
    for row in reversed(range(order)):
        total = middle[row]
        for inner in range(row + 1, order):
            total = total - lower[inner][row] * result[inner]
        result[row] = total / lower[row][row]
    return jnp.stack(result)

def reference(rbf_blocks, fluid_traction, fluid_mass, route, slot, shell_inverse, robin_coef, shell_start):
    groups = N_FLUID * N_SOLID
    breadth = 3 * NODES
    shells_all = shell_start.shape[0]
    target = (route[:, 0] * SB_DEV + slot).astype(jnp.int32)
    rbf_grouped = rbf_blocks.reshape(groups, FB_DEV, NODES, NODES)
    traction_grouped = fluid_traction.reshape(groups, FB_DEV, breadth)
    mass_grouped = fluid_mass.reshape(groups, FB_DEV, breadth)
    inverse_grouped = shell_inverse.reshape(groups, SB_DEV, breadth, breadth)
    count = shells_all * breadth
    batching = min(16, groups)
    current = shell_start
    residuals = []
    images = []
    norms = []
    last_load = None
    for iteration in range(ITERS):
        displaced = current.astype(jnp.bfloat16)[target]
        loads, mapped = lax.map(fluid_side, (rbf_grouped, displaced.reshape(groups, FB_DEV, breadth), traction_grouped, mass_grouped), batch_size=batching)
        last_load = loads.reshape(-1, breadth)
        shell_load = jax.ops.segment_sum(mapped.reshape(-1, breadth).astype(jnp.float32), target, num_segments=shells_all)
        forcing = (shell_load + robin_coef * current).astype(jnp.bfloat16)
        image = lax.map(shell_side, (inverse_grouped, forcing.reshape(groups, SB_DEV, breadth)), batch_size=batching).reshape(shells_all, breadth)
        residual = image - current
        squares = jnp.sum(residual * residual)
        norms.append(jnp.sqrt(squares / count + EPSILON))
        residuals.append(residual)
        images.append(image)
        if iteration == 0:
            current = current + RELAX * residual
        else:
            changes = jnp.stack([(residuals[i + 1] - residuals[i]).reshape(-1) for i in range(iteration)])
            image_changes = jnp.stack([images[i + 1] - images[i] for i in range(iteration)])
            gram = jnp.dot(changes, changes.T, precision=lax.Precision.HIGHEST)
            rhs = jnp.dot(changes, residual.reshape(-1), precision=lax.Precision.HIGHEST)
            coefs = least_squares(gram, -rhs)
            current = image + jnp.tensordot(coefs, image_changes, axes=1, precision=lax.Precision.HIGHEST)
    return (current, last_load, jnp.stack(norms))
```

```python
import functools

import jax
import jax.numpy as jnp
from jax import lax
from jax.experimental import pallas as pl
from jax.experimental.pallas import tpu as pltpu
from jax.sharding import PartitionSpec as P

ITERS = 6


RELAX = 0.3
EPSILON = 1e-06


def transport(buffer, devices, capacity):
    breadth = buffer.shape[1]
    moved = lax.all_to_all(
        buffer.reshape(devices, capacity, breadth),
        ("fluid", "solid"),
        split_axis=0,
        concat_axis=0,
        tiled=True,
    )
    return moved.reshape(devices * capacity, breadth)


def least_squares(gram, target_side):
    order = gram.shape[0]
    lower = [[None] * order for _ in range(order)]
    for row in range(order):
        for column in range(row + 1):
            total = gram[row, column]
            for inner in range(column):
                total = total - lower[row][inner] * lower[column][inner]
            if row == column:
                lower[row][row] = jnp.sqrt(total)
            else:
                lower[row][column] = total / lower[column][column]
    middle = []
    for row in range(order):
        total = target_side[row]
        for inner in range(row):
            total = total - lower[row][inner] * middle[inner]
        middle.append(total / lower[row][row])
    result = [None] * order
    for row in reversed(range(order)):
        total = middle[row]
        for inner in range(row + 1, order):
            total = total - lower[inner][row] * result[inner]
        result[row] = total / lower[row][row]
    return jnp.stack(result)


def per_device(
    rbf_blocks, fluid_traction, fluid_mass, route, slot, shell_inverse, robin_coef, shell_start
):
    devices = lax.axis_size("fluid") * lax.axis_size("solid")
    blocks = rbf_blocks.shape[0]
    nodes = rbf_blocks.shape[1]
    breadth = 3 * nodes
    shells = shell_inverse.shape[0]
    capacity = max(2, 2 * blocks // devices)
    slots_all = devices * capacity
    destination = route[:, 0]
    block_order = jnp.arange(blocks, dtype=jnp.int32)
    earlier = (destination[:, None] == destination[None, :]) & (
        block_order[None, :] < block_order[:, None]
    )
    slot_rank = jnp.sum(earlier.astype(jnp.int32), axis=1)
    position = destination * capacity + slot_rank
    positions = jnp.arange(slots_all, dtype=jnp.int32)
    placing = positions[:, None] == position[None, :]
    place_out = placing.astype(jnp.bfloat16)
    place_in = (position[:, None] == positions[None, :]).astype(jnp.bfloat16)
    wanted = jnp.max(jnp.where(placing, slot[None, :] + 1, 0), axis=1) - 1
    asked = lax.all_to_all(
        wanted.reshape(devices, capacity),
        ("fluid", "solid"),
        split_axis=0,
        concat_axis=0,
        tiled=True,
    ).reshape(slots_all)
    shell_ids = jnp.arange(shells, dtype=jnp.int32)
    picking = (asked[:, None] == shell_ids[None, :]).astype(jnp.bfloat16)
    collecting = (shell_ids[:, None] == asked[None, :]).astype(jnp.bfloat16)
    traction = fluid_traction.astype(jnp.float32)
    massive = fluid_mass.astype(jnp.float32)
    count = shells * devices * breadth
    current = shell_start
    residuals = []
    images = []
    norms = []
    last_load = None
    for iteration in range(ITERS):
        current_half = current.astype(jnp.bfloat16)
        outgoing = jnp.dot(picking, current_half, preferred_element_type=jnp.float32).astype(
            jnp.bfloat16
        )
        incoming = transport(outgoing, devices, capacity)
        displaced = jnp.dot(place_in, incoming, preferred_element_type=jnp.float32).astype(
            jnp.bfloat16
        )
        moved = jnp.einsum(
            "bcj,bij->bci",
            displaced.reshape(blocks, 3, nodes),
            rbf_blocks,
            preferred_element_type=jnp.float32,
        ).reshape(blocks, breadth)
        load = (traction - massive * moved).astype(jnp.bfloat16)
        last_load = load
        mapped = (
            jnp.einsum(
                "bci,bij->bcj",
                load.reshape(blocks, 3, nodes),
                rbf_blocks,
                preferred_element_type=jnp.float32,
            )
            .reshape(blocks, breadth)
            .astype(jnp.bfloat16)
        )
        sending = jnp.dot(place_out, mapped, preferred_element_type=jnp.float32).astype(
            jnp.bfloat16
        )
        arrived = transport(sending, devices, capacity)
        shell_load = jnp.dot(collecting, arrived, preferred_element_type=jnp.float32)
        forcing = (shell_load + robin_coef * current).astype(jnp.bfloat16)
        image = jnp.einsum("bi,bij->bj", forcing, shell_inverse, preferred_element_type=jnp.float32)
        residual = image - current
        residuals.append(residual)
        images.append(image)
        squares_local = jnp.sum(residual * residual)
        if iteration == 0:
            gram_local = jnp.zeros((1, 1), jnp.float32)
            rhs_local = jnp.zeros((1,), jnp.float32)
        else:
            changes = jnp.stack(
                [(residuals[i + 1] - residuals[i]).reshape(-1) for i in range(iteration)]
            )
            gram_local = jnp.dot(changes, changes.T, precision=lax.Precision.HIGHEST)
            rhs_local = jnp.dot(changes, residual.reshape(-1), precision=lax.Precision.HIGHEST)
        gram, rhs, squares = lax.psum((gram_local, rhs_local, squares_local), ("fluid", "solid"))
        norms.append(jnp.sqrt(squares / count + EPSILON))
        if iteration == 0:
            current = current + RELAX * residual
        else:
            image_changes = jnp.stack([images[i + 1] - images[i] for i in range(iteration)])
            coefs = least_squares(gram, -rhs)
            current = image + jnp.tensordot(
                coefs, image_changes, axes=1, precision=lax.Precision.HIGHEST
            )
    return (current, last_load, jnp.stack(norms))


CHUNK = 8
LANES = 128
VMEM_BYTES = 67043328
MESH = pl.DeviceIdType.MESH


def kernel(
    nf, nz, blocks, nodes, shells, count,
    key_ref, row_ref, tr_ref, ms_ref, robin_ref, start_ref, rbf_hbm, inv_hbm,
    cur_out, load_out, norm_out,
    rbf, inv, slots, curb, cur_own, vhist, rprev, sc, place, collect, disp, loadf, mapped,
    part, send_a, recv_a, send_b, recv_b, send_c, recv_c, shell_sum,
    rbf_sem, inv_sem,
    s1, r1, s2, r2, s3, r3, sa, ra, sb, rb, sc_s, sc_r,
):
    f32, bf16 = jnp.float32, jnp.bfloat16
    breadth = 3 * nodes
    nxy = nf // 2
    group = nz * shells
    every = nf * group
    f = lax.axis_index("fluid")
    z = lax.axis_index("solid")
    xy = f // 2
    core = lax.rem(f, 2)
    other = 1 - core
    nchunk = blocks // CHUNK
    rows = disp.shape[0]

    def turn(value, step, size):
        return lax.rem(value + step + size, size)

    def fluid_of(plane, unit):
        return plane * 2 + unit

    def first_row(plane, unit, depth):
        return pl.multiple_of((fluid_of(plane, unit) * nz + depth) * shells, shells)

    def rbf_copy(i):
        at = pl.ds(i * CHUNK, CHUNK)
        return pltpu.make_async_copy(rbf_hbm.at[at], rbf.at[at], rbf_sem.at[i])

    def inv_copy():
        return pltpu.make_async_copy(inv_hbm, inv, inv_sem)

    def start_rbf(i, carry):
        rbf_copy(i).start()
        return carry

    lax.fori_loop(0, nchunk, start_rbf, 0)
    inv_copy().start()

    own_row = first_row(xy, core, z)
    for j in range(ITERS + 1):
        slots[j] = jnp.zeros(slots.shape[1:], f32)
    slots[0, pl.ds(own_row, shells), 0:breadth] = start_ref[...]
    vhist[...] = jnp.zeros(vhist.shape, f32)
    sc[...] = jnp.zeros(sc.shape, f32)
    rprev[...] = jnp.zeros(rprev.shape, f32)
    mapped[...] = jnp.zeros(mapped.shape, f32)
    loadf[...] = jnp.zeros(loadf.shape, f32)

    barrier = pltpu.get_barrier_semaphore()
    for d in range(1, nz):
        pl.semaphore_signal(barrier, inc=1, device_id=(f, turn(z, d, nz)), device_id_type=MESH)
    for e in range(1, nxy):
        pl.semaphore_signal(
            barrier, inc=1, device_id=(fluid_of(turn(xy, e, nxy), core), z), device_id_type=MESH
        )
    pl.semaphore_signal(barrier, inc=1, device_id=(fluid_of(xy, other), z), device_id_type=MESH)

    place[...] = jnp.where(
        key_ref[...] == lax.broadcasted_iota(jnp.int32, (rows, 3 * every), 1), 1.0, 0.0
    ).astype(bf16)
    for side in range(2):
        unit = core if side == 0 else other
        line = lax.broadcasted_iota(jnp.int32, (nxy * group, 1), 0)
        ids = (line // group * 2 + unit) * group + lax.rem(line, group)
        for c in range(3):
            collect[side, c] = jnp.where(ids + c * every == row_ref[...], 1.0, 0.0).astype(bf16)

    pl.semaphore_wait(barrier, (nz - 1) + (nxy - 1) + 1)

    def all_gather(j, lanes):
        def block(plane, unit, depth):
            return slots.at[j, pl.ds(first_row(plane, unit, depth), shells), lanes]

        def send(ref, send_sem, recv_sem, fluid, solid):
            return pltpu.make_async_remote_copy(
                src_ref=ref, dst_ref=ref, send_sem=send_sem, recv_sem=recv_sem,
                device_id=(fluid, solid), device_id_type=MESH,
            )

        def along(d, incoming=False):
            depth = turn(z, -d, nz) if incoming else z
            return send(block(xy, core, depth), s1.at[d - 1], r1.at[d - 1], f, turn(z, d, nz))

        def across(d, e, incoming=False):
            plane = turn(xy, -e, nxy) if incoming else xy
            return send(
                block(plane, core, turn(z, -d, nz)), s2.at[d, e - 1], r2.at[d, e - 1],
                fluid_of(turn(xy, e, nxy), core), z,
            )

        def pair(d, e, incoming=False):
            unit = other if incoming else core
            return send(
                block(turn(xy, -e, nxy), unit, turn(z, -d, nz)), s3.at[d, e], r3.at[d, e],
                fluid_of(xy, other), z,
            )

        for d in range(1, nz):
            along(d).start()
        for d in range(nz):
            if d > 0:
                along(d, True).wait_recv()
            for e in range(1, nxy):
                across(d, e).start()
            pair(d, 0).start()
        for d in range(nz):
            for e in range(1, nxy):
                across(d, e, True).wait_recv()
                pair(d, e).start()
        for d in range(nz):
            for e in range(nxy):
                pair(d, e, True).wait_recv()
        for d in range(1, nz):
            along(d).wait_send()
        for d in range(nz):
            for e in range(1, nxy):
                across(d, e).wait_send()
            for e in range(nxy):
                pair(d, e).wait_send()

    lane = lax.broadcasted_iota(jnp.int32, (1, LANES), 1)

    def pick(vector, q):
        return jnp.sum(jnp.where(lane == q, vector, 0.0), axis=1, keepdims=True)

    def coefficients(j):
        k = j - 1
        total = jnp.sum(slots[j, :, breadth:], axis=0, keepdims=True)
        sc[j] = total
        norm = jnp.sqrt(pick(total, 0) / count + EPSILON)

        @pl.when(j > 0)
        def _():
            norm_out[jnp.maximum(k, 0)] = jnp.broadcast_to(norm, (1, LANES))

        order = ITERS - 1
        gram = [[None] * order for _ in range(order)]
        for col in range(order):
            vector = sc[col + 2]
            for row in range(col + 1):
                value = pick(vector, 8 + row)
                if row == col:
                    value = jnp.where(col < k, value, 1.0)
                gram[col][row] = value
        side = [-pick(total, 1 + i) for i in range(order)]
        lower = [[None] * order for _ in range(order)]
        for row in range(order):
            for col in range(row + 1):
                value = gram[row][col]
                for inner in range(col):
                    value = value - lower[row][inner] * lower[col][inner]
                if row == col:
                    lower[row][row] = jnp.sqrt(value)
                else:
                    lower[row][col] = value / lower[col][col]
        middle = []
        for row in range(order):
            value = side[row]
            for inner in range(row):
                value = value - lower[row][inner] * middle[inner]
            middle.append(value / lower[row][row])
        result = [None] * order
        for row in reversed(range(order)):
            value = middle[row]
            for inner in range(row + 1, order):
                value = value - lower[inner][row] * result[inner]
            result[row] = value / lower[row][row]
        relax = jnp.where(j == 1, jnp.full((1, 1), RELAX - 1.0, f32), 0.0)
        return [relax] + result

    def combine(j, coefs, at):
        value = slots[j, at, 0:breadth]
        before = slots[0, at, 0:breadth]
        for i in range(ITERS):
            after = slots[i + 1, at, 0:breadth]
            value = value + coefs[i] * (after - before)
            before = after
        return value

    def dot(a, b, dims=((1,), (0,))):
        return lax.dot_general(a, b, (dims, ((), ())), preferred_element_type=f32)

    def iteration(j, carry):
        all_gather(j, pl.ds(0, breadth + LANES))
        coefs = coefficients(j)

        def update(i, c):
            at = pl.ds(pl.multiple_of(i * 16, 16), 16)
            curb[at, :] = combine(j, coefs, at).astype(bf16)
            return c

        lax.fori_loop(0, every // 16, update, 0)
        cur_own[...] = combine(j, coefs, pl.ds(own_row, shells))
        picked = None
        for c in range(3):
            term = dot(
                place[:, c * every:(c + 1) * every], curb[:, c * nodes:(c + 1) * nodes]
            )
            picked = term if picked is None else picked + term
        disp[...] = picked

        def fluid(i, c):
            @pl.when(j == 0)
            def _():
                rbf_copy(i).wait()

            loads = []
            for u in range(CHUNK):
                b = i * CHUNK + u
                at = pl.ds(pl.multiple_of(b * 8, 8), 8)
                moved = dot(disp[at, :].astype(bf16), rbf[b], ((1,), (1,)))
                load = (tr_ref[at, :] - ms_ref[at, :] * moved).astype(bf16)
                loadf[at, :] = load.astype(f32)
                loads.append(load)
            for u in range(CHUNK):
                b = i * CHUNK + u
                at = pl.ds(pl.multiple_of(b * 8, 8), 8)
                mapped[at, :] = dot(loads[u], rbf[b]).astype(bf16).astype(f32)
            return c

        lax.fori_loop(0, nchunk, fluid, 0)

        mapped_half = mapped[...].astype(bf16)
        for c in range(3):
            send_a[:, c * nodes:(c + 1) * nodes] = dot(collect[1, c], mapped_half).astype(bf16)
        copy_a = pltpu.make_async_remote_copy(
            src_ref=send_a, dst_ref=recv_a, send_sem=sa, recv_sem=ra,
            device_id=(fluid_of(xy, other), z), device_id_type=MESH,
        )
        copy_a.start()
        for c in range(3):
            part[:, c * nodes:(c + 1) * nodes] = dot(collect[0, c], mapped_half)
        copy_a.wait_recv()
        part[...] = part[...] + recv_a[...].astype(f32)

        def copy_b(e):
            return pltpu.make_async_remote_copy(
                src_ref=send_b.at[e - 1], dst_ref=recv_b.at[e - 1],
                send_sem=sb.at[e - 1], recv_sem=rb.at[e - 1],
                device_id=(fluid_of(turn(xy, e, nxy), core), z), device_id_type=MESH,
            )

        for e in range(1, nxy):
            at = pl.ds(pl.multiple_of(turn(xy, e, nxy) * group, group), group)
            send_b[e - 1] = part[at, :].astype(bf16)
            copy_b(e).start()
        line = part[pl.ds(pl.multiple_of(xy * group, group), group), :]
        for e in range(1, nxy):
            copy_b(e).wait_recv()
            line = line + recv_b[e - 1].astype(f32)
        shell_sum[...] = line

        def copy_c(d):
            return pltpu.make_async_remote_copy(
                src_ref=send_c.at[d - 1], dst_ref=recv_c.at[d - 1],
                send_sem=sc_s.at[d - 1], recv_sem=sc_r.at[d - 1],
                device_id=(f, turn(z, d, nz)), device_id_type=MESH,
            )

        for d in range(1, nz):
            at = pl.ds(pl.multiple_of(turn(z, d, nz) * shells, shells), shells)
            send_c[d - 1] = shell_sum[at, :].astype(bf16)
            copy_c(d).start()
        shell_load = shell_sum[pl.ds(pl.multiple_of(z * shells, shells), shells), :]
        for d in range(1, nz):
            copy_c(d).wait_recv()
            shell_load = shell_load + recv_c[d - 1].astype(f32)
        copy_a.wait_send()
        for e in range(1, nxy):
            copy_b(e).wait_send()
        for d in range(1, nz):
            copy_c(d).wait_send()

        @pl.when(j == 0)
        def _():
            inv_copy().wait()

        current = cur_own[...]
        forcing = (shell_load + robin_ref[...] * current).astype(bf16)
        shell_row = lax.broadcasted_iota(jnp.int32, (shells, breadth), 0)

        def solid(s, image):
            return jnp.where(shell_row == s, dot(forcing, inv[s]), image)

        image = lax.fori_loop(0, shells, solid, jnp.zeros((shells, breadth), f32))
        residual = image - current
        newest = residual - rprev[...]
        rprev[...] = residual
        vhist[lax.rem(j + ITERS - 1, ITERS)] = newest
        lane_rows = lax.broadcasted_iota(jnp.int32, (shells, LANES), 1)

        def put(vector, q, product):
            return jnp.where(lane_rows == q, jnp.sum(product, axis=1, keepdims=True), vector)

        scalars = put(jnp.zeros((shells, LANES), f32), 0, residual * residual)
        for i in range(ITERS - 1):
            scalars = put(scalars, 1 + i, vhist[i] * residual)
            scalars = put(scalars, 8 + i, vhist[i] * newest)
        own = pl.ds(own_row, shells)
        slots[j + 1, own, 0:breadth] = image
        slots[j + 1, own, breadth:] = scalars
        return carry

    lax.fori_loop(0, ITERS, iteration, 0)
    all_gather(ITERS, pl.ds(breadth, LANES))
    cur_out[...] = combine(ITERS, coefficients(ITERS), pl.ds(own_row, shells))
    load_out[...] = loadf[0:blocks * 8, :].astype(bf16)


def fused(nf, nz, rbf_blocks, fluid_traction, fluid_mass, route, slot, shell_inverse, robin_coef, shell_start):
    f32, bf16 = jnp.float32, jnp.bfloat16
    blocks, nodes, _ = rbf_blocks.shape
    shells, breadth = shell_start.shape
    nxy = nf // 2
    group = nz * shells
    every = nf * group
    rows = -(-blocks * 8 // LANES) * LANES
    target = route[:, 0] * shells + slot
    part_of = jnp.arange(8, dtype=jnp.int32)[None, :]
    key = jnp.where(part_of < 3, target[:, None] + part_of * every, -1).reshape(-1)
    key = jnp.pad(key, (0, rows - blocks * 8), constant_values=-1)

    def spread(x):
        return jnp.pad(
            x.reshape(blocks, 3, nodes).astype(f32), ((0, 0), (0, 5), (0, 0))
        ).reshape(blocks * 8, nodes)

    dma = pltpu.SemaphoreType.DMA
    vmem = pl.BlockSpec(memory_space=pltpu.VMEM)
    anywhere = pl.BlockSpec(memory_space=pl.ANY)
    current, load, norms = pl.pallas_call(
        functools.partial(kernel, nf, nz, blocks, nodes, shells, every * breadth),
        out_shape=(
            jax.ShapeDtypeStruct((shells, breadth), f32),
            jax.ShapeDtypeStruct((blocks * 8, nodes), bf16),
            jax.ShapeDtypeStruct((ITERS, 1, LANES), f32),
        ),
        in_specs=[vmem] * 6 + [anywhere] * 2,
        out_specs=(vmem, vmem, vmem),
        scratch_shapes=[
            pltpu.VMEM(rbf_blocks.shape, bf16),
            pltpu.VMEM(shell_inverse.shape, bf16),
            pltpu.VMEM((ITERS + 1, every, breadth + LANES), f32),
            pltpu.VMEM((every, breadth), bf16),
            pltpu.VMEM((shells, breadth), f32),
            pltpu.VMEM((ITERS, shells, breadth), f32),
            pltpu.VMEM((shells, breadth), f32),
            pltpu.VMEM((ITERS + 1, 1, LANES), f32),
            pltpu.VMEM((rows, 3 * every), bf16),
            pltpu.VMEM((2, 3, nxy * group, rows), bf16),
            pltpu.VMEM((rows, nodes), f32),
            pltpu.VMEM((rows, nodes), f32),
            pltpu.VMEM((rows, nodes), f32),
            pltpu.VMEM((nxy * group, breadth), f32),
            pltpu.VMEM((nxy * group, breadth), bf16),
            pltpu.VMEM((nxy * group, breadth), bf16),
            pltpu.VMEM((nxy - 1, group, breadth), bf16),
            pltpu.VMEM((nxy - 1, group, breadth), bf16),
            pltpu.VMEM((nz - 1, shells, breadth), bf16),
            pltpu.VMEM((nz - 1, shells, breadth), bf16),
            pltpu.VMEM((group, breadth), f32),
            dma((blocks // CHUNK,)),
            dma,
            dma((nz - 1,)), dma((nz - 1,)),
            dma((nz, nxy - 1)), dma((nz, nxy - 1)),
            dma((nz, nxy)), dma((nz, nxy)),
            dma, dma,
            dma((nxy - 1,)), dma((nxy - 1,)),
            dma((nz - 1,)), dma((nz - 1,)),
        ],
        compiler_params=pltpu.CompilerParams(
            collective_id=0, has_side_effects=True, vmem_limit_bytes=VMEM_BYTES
        ),
        name="coupling",
    )(
        key[:, None], key[None, :], spread(fluid_traction), spread(fluid_mass),
        robin_coef, shell_start, rbf_blocks, shell_inverse,
    )
    load = load.reshape(blocks, 8, nodes)[:, :3].reshape(blocks, breadth)
    return current, load, norms[:, 0, 0]


def choose(nf, nz):
    def body(rbf_blocks, *others):
        if nf * nz > 32:
            return per_device(rbf_blocks, *others)
        return fused(nf, nz, rbf_blocks, *others)

    return body


def solution(mesh):
    in_specs = (
        P(("fluid", "solid"), None, None),
        P(("fluid", "solid"), None),
        P(("fluid", "solid"), None),
        P(("fluid", "solid"), None),
        P(("fluid", "solid")),
        P(("fluid", "solid"), None, None),
        P(("fluid", "solid"), None),
        P(("fluid", "solid"), None),
    )
    out_specs = (P(("fluid", "solid"), None), P(("fluid", "solid"), None), P())
    return jax.shard_map(
        choose(mesh.shape["fluid"], mesh.shape["solid"]), mesh=mesh, in_specs=in_specs, out_specs=out_specs, check_vma=False
    )
```
